16 devices in a mesh: ep: 16 (over z, y, x, core).
Axes of the slice: x: 2, y: 2, z: 2, core: 2. Of those that a mesh axis runs over, the one named last changes fastest.
Arguments:
- tokens: bfloat16 [8192, 256], P('ep')
- grad_out: bfloat16 [8192, 256], P('ep')
- expert_ids: int32 [8192, 2], P('ep')
- w_gate: bfloat16 [256, 16], replicated
- w_in: bfloat16 [16, 256, 1024], P('ep')
- w_out: bfloat16 [16, 1024, 256], P('ep')
Outputs:
- output 1: bfloat16 [8192, 256], P('ep')
- output 2: bfloat16 [8192, 256], P('ep')
- output 3: float32 [16, 256, 1024], P('ep')
- output 4: float32 [16, 1024, 256], P('ep')
- output 5: float32 [256, 16], replicated
All inputs are finite; a program needn't handle non-finite values.
Results may differ from the reference program's by a relative error of at most 0.00491079.
Values are sent between devices in bfloat16 or wider.
A program may use at most 1 GiB of HBM per device.

```python
import jax
import jax.numpy as jnp
from jax import lax

EXPERTS = 16
TOKENS_DEV = 512
D_MODEL = 256
D_HIDDEN = 1024
HOT_EXPERTS = 3

CAP_ROWS = TOKENS_DEV // 4
ALL_TOKENS = EXPERTS * TOKENS_DEV
CAP_ALL = EXPERTS * CAP_ROWS


def draw_routes(route_key):
    k_perm, k_shift, k_order, k_swap = jax.random.split(route_key, 4)
    n_cold = EXPERTS - HOT_EXPERTS
    cold_choices = 2 * TOKENS_DEV - HOT_EXPERTS * CAP_ROWS
    slot_pos = jnp.arange(2 * TOKENS_DEV)
    hot_rank = jnp.minimum(slot_pos // CAP_ROWS, HOT_EXPERTS - 1)
    cold_block = (jnp.maximum(slot_pos - HOT_EXPERTS * CAP_ROWS, 0) * n_cold) // cold_choices
    shifts = jax.random.randint(k_shift, (EXPERTS, 1), 0, n_cold)
    cold_rank = HOT_EXPERTS + (cold_block[None, :] + shifts) % n_cold
    rank_ids = jnp.where(slot_pos[None, :] < HOT_EXPERTS * CAP_ROWS, hot_rank[None, :], cold_rank)
    expert_perm = jax.random.permutation(k_perm, EXPERTS)
    choice_ids = expert_perm[rank_ids]
    pair_ids = jnp.stack([choice_ids[:, :TOKENS_DEV], choice_ids[:, TOKENS_DEV:]], axis=-1)
    token_perm = jax.random.permutation(k_order, jnp.tile(jnp.arange(TOKENS_DEV), (EXPERTS, 1)), axis=1, independent=True)
    pair_ids = jnp.take_along_axis(pair_ids, token_perm[:, :, None], axis=1)
    swap_bit = jax.random.randint(k_swap, (EXPERTS, TOKENS_DEV, 1), 0, 2)
    pair_ids = jnp.where(swap_bit == 1, pair_ids[:, :, ::-1], pair_ids)
    return pair_ids.reshape(ALL_TOKENS, 2).astype(jnp.int32)


def setup_inputs(seed: int = 0) -> dict:
    rng_key = jax.random.key(seed)
    k_tok, k_grad, k_route, k_gate, k_in, k_out = jax.random.split(rng_key, 6)
    tokens = jax.random.normal(k_tok, (ALL_TOKENS, D_MODEL), jnp.float32).astype(jnp.bfloat16)
    grad_out = jax.random.normal(k_grad, (ALL_TOKENS, D_MODEL), jnp.float32).astype(jnp.bfloat16)
    expert_ids = draw_routes(k_route)
    w_gate = (jax.random.normal(k_gate, (D_MODEL, EXPERTS), jnp.float32) * D_MODEL ** -0.5).astype(jnp.bfloat16)
    w_in = (jax.random.normal(k_in, (EXPERTS, D_MODEL, D_HIDDEN), jnp.float32) * D_MODEL ** -0.5).astype(jnp.bfloat16)
    w_out = (jax.random.normal(k_out, (EXPERTS, D_HIDDEN, D_MODEL), jnp.float32) * D_HIDDEN ** -0.5).astype(jnp.bfloat16)
    return {'tokens': tokens, 'grad_out': grad_out, 'expert_ids': expert_ids, 'w_gate': w_gate, 'w_in': w_in, 'w_out': w_out}


def reference(tokens, grad_out, expert_ids, w_gate, w_in, w_out):
    n_choice = 2 * ALL_TOKENS
    logits = jnp.dot(tokens, w_gate, preferred_element_type=jnp.float32)
    prob_all = jax.nn.softmax(logits, axis=-1)
    picked = jnp.take_along_axis(prob_all, expert_ids, axis=1)
    gate_val = picked / jnp.sum(picked, axis=1, keepdims=True)
    flat_ids = expert_ids.reshape(-1)
    sort_order = jnp.argsort(flat_ids, stable=True)
    counts = jnp.bincount(flat_ids, length=EXPERTS)
    starts = jnp.cumsum(counts) - counts
    pad_rows = jnp.zeros((CAP_ALL, D_MODEL), jnp.bfloat16)
    x_sorted = jnp.concatenate([tokens[sort_order // 2], pad_rows], axis=0)
    dy_flat = (gate_val[:, :, None] * grad_out[:, None, :].astype(jnp.float32)).astype(jnp.bfloat16).reshape(n_choice, D_MODEL)
    dy_sorted = jnp.concatenate([dy_flat[sort_order], pad_rows], axis=0)
    row_iota = jnp.arange(CAP_ALL)[:, None]

    def expert_step(scan_carry, per_expert):
        y_acc, dx_acc = scan_carry
        w_one, w_two, start_row, row_count = per_expert
        keep_row = row_iota < row_count
        x_rows = jnp.where(keep_row, lax.dynamic_slice_in_dim(x_sorted, start_row, CAP_ALL), 0)
        dy_rows = jnp.where(keep_row, lax.dynamic_slice_in_dim(dy_sorted, start_row, CAP_ALL), 0)
        a_pre = jnp.dot(x_rows, w_one, preferred_element_type=jnp.float32)
        hidden, gelu_vjp = jax.vjp(jax.nn.gelu, a_pre)
        hid_b = hidden.astype(jnp.bfloat16)
        y_rows = jnp.dot(hid_b, w_two, preferred_element_type=jnp.float32).astype(jnp.bfloat16)
        g_two = jnp.dot(hid_b.T, dy_rows, preferred_element_type=jnp.float32)
        d_hid = jnp.dot(dy_rows, w_two.T, preferred_element_type=jnp.float32)
        d_pre = gelu_vjp(d_hid)[0].astype(jnp.bfloat16)
        g_one = jnp.dot(x_rows.T, d_pre, preferred_element_type=jnp.float32)
        dx_rows = jnp.dot(d_pre, w_one.T, preferred_element_type=jnp.float32).astype(jnp.bfloat16)
        y_acc = lax.dynamic_update_slice_in_dim(y_acc, lax.dynamic_slice_in_dim(y_acc, start_row, CAP_ALL) + y_rows.astype(jnp.float32), start_row, axis=0)
        dx_acc = lax.dynamic_update_slice_in_dim(dx_acc, lax.dynamic_slice_in_dim(dx_acc, start_row, CAP_ALL) + dx_rows.astype(jnp.float32), start_row, axis=0)
        return (y_acc, dx_acc), (g_one, g_two)

    acc_init = jnp.zeros((n_choice + CAP_ALL, D_MODEL), jnp.float32)
    acc_done, grads = lax.scan(expert_step, (acc_init, acc_init), (w_in, w_out, starts, counts))
    g_in, g_out = grads
    y_sorted = acc_done[0][:n_choice]
    dx_sorted = acc_done[1][:n_choice]
    y_pair = jnp.zeros_like(y_sorted).at[sort_order].set(y_sorted).reshape(ALL_TOKENS, 2, D_MODEL)
    dx_pair = jnp.zeros_like(dx_sorted).at[sort_order].set(dx_sorted).reshape(ALL_TOKENS, 2, D_MODEL)
    y_out = jnp.sum(gate_val[:, :, None] * y_pair, axis=1).astype(jnp.bfloat16)
    d_gate = jnp.sum(grad_out.astype(jnp.float32)[:, None, :] * y_pair, axis=-1)
    d_sel = gate_val * (d_gate - jnp.sum(gate_val * d_gate, axis=1, keepdims=True))
    choice_hot = expert_ids[:, :, None] == jnp.arange(EXPERTS)[None, None, :]
    d_logits = jnp.sum(jnp.where(choice_hot, d_sel[:, :, None], 0.0), axis=1).astype(jnp.bfloat16)
    grad_x = (jnp.sum(dx_pair, axis=1) + jnp.dot(d_logits, w_gate.T, preferred_element_type=jnp.float32)).astype(jnp.bfloat16)
    grad_w_gate = jnp.dot(tokens.T, d_logits, preferred_element_type=jnp.float32)
    return y_out, grad_x, g_in, g_out, grad_w_gate
```

```python
import functools

import jax
import jax.numpy as jnp
from jax import lax
from jax.experimental import pallas as pl
from jax.experimental.pallas import tpu as pltpu
from jax.sharding import PartitionSpec as P

N = 16
CAP = 128
TOK = 512
D = 256
H = 1024
MESH = pl.DeviceIdType.MESH
F32 = jnp.float32
BF16 = jnp.bfloat16
GELU_C = 0.7978845608028654
GELU_A = 0.044715


def peer_of(me, k):
    out = me
    for bit in (1, 2, 4, 8):
        mine = (me // bit) % 2
        flip = (k // bit) % 2
        out = out + flip * bit * (1 - 2 * mine)
    return out


def nn(a, b):
    return lax.dot_general(a, b, (((1,), (0,)), ((), ())), preferred_element_type=F32)


def nt(a, b):
    return lax.dot_general(a, b, (((1,), (1,)), ((), ())), preferred_element_type=F32)


def tn(a, b):
    return lax.dot_general(a, b, (((0,), (0,)), ((), ())), preferred_element_type=F32)


def kernel(x_ref, do_ref, ids_ref, wg_ref, w1_hbm, w2_hbm,
           y_ref, gx_ref, gwi_hbm, gwo_hbm, gwg_ref,
           w1, w2, send, recv, ys, yr, dxs, dxr, hid, dpre, gwi, gwo,
           slot_row, gate_row, slot_col, gate_col, acc_y, acc_dx, acc_dg, gbuf,
           in_s, in_r, y_s, y_r, dx_s, dx_r, g_s, g_r, loc):
    me = lax.axis_index('ep')

    def rcopy(src, dst, s_sem, r_sem, k):
        return pltpu.make_async_remote_copy(src_ref=src, dst_ref=dst, send_sem=s_sem, recv_sem=r_sem, device_id=(peer_of(me, k),), device_id_type=MESH)

    def in_copy(k):
        return rcopy(send.at[k], recv.at[k], in_s.at[k], in_r.at[k], k)

    def y_copy(k):
        return rcopy(ys.at[k], yr.at[k], y_s.at[k], y_r.at[k], k)

    def dx_copy(k):
        return rcopy(dxs.at[k], dxr.at[k], dx_s.at[k], dx_r.at[k], k)

    barrier = pltpu.get_barrier_semaphore()

    @pl.loop(1, N)
    def _(k):
        pl.semaphore_signal(barrier, inc=1, device_id=(peer_of(me, k),), device_id_type=MESH)

    w1_in = pltpu.make_async_copy(w1_hbm, w1, loc.at[0])
    w2_in = pltpu.make_async_copy(w2_hbm, w2, loc.at[1])
    w1_in.start()
    w2_in.start()

    x = x_ref[...]
    logits = nt(wg_ref[...], x)
    id0 = ids_ref[0:1, :]
    id1 = ids_ref[1:2, :]
    exp_iota = lax.broadcasted_iota(jnp.int32, (N, TOK), 0)
    l0 = jnp.sum(jnp.where(exp_iota == id0, logits, 0.0), axis=0, keepdims=True)
    l1 = jnp.sum(jnp.where(exp_iota == id1, logits, 0.0), axis=0, keepdims=True)
    top = jnp.maximum(l0, l1)
    e0 = jnp.exp(l0 - top)
    e1 = jnp.exp(l1 - top)
    g0 = e0 / (e0 + e1)
    g1 = e1 / (e0 + e1)
    peer_iota = jnp.bitwise_xor(exp_iota, me)
    hot0 = peer_iota == id0
    hot1 = peer_iota == id1
    named = jnp.logical_or(hot0, hot1)
    row_i = lax.broadcasted_iota(jnp.int32, (TOK, TOK), 0)
    col_i = lax.broadcasted_iota(jnp.int32, (TOK, TOK), 1)
    before = jnp.where(row_i < col_i, 1.0, 0.0).astype(BF16)
    rank = nn(jnp.where(named, 1.0, 0.0).astype(BF16), before)
    slots = jnp.where(named, rank, -1.0)
    gates = jnp.where(hot0, g0, 0.0) + jnp.where(hot1, g1, 0.0)
    slot_row[...] = slots
    gate_row[...] = gates

    pl.semaphore_wait(barrier, N - 1)

    slot_iota = lax.broadcasted_iota(jnp.int32, (CAP, TOK), 0).astype(F32)

    def fill(k):
        hit = slot_iota == slot_row[pl.ds(k, 1), :]
        sel = jnp.where(hit, 1.0, 0.0).astype(BF16)
        g_slot = jnp.sum(jnp.where(hit, gate_row[pl.ds(k, 1), :], 0.0), axis=1, keepdims=True)
        return nn(sel, x_ref[...]).astype(BF16), (g_slot * nn(sel, do_ref[...])).astype(BF16)

    @pl.loop(1, N)
    def _(k):
        xs, dys = fill(k)
        send[k, :, 0:D] = xs
        send[k, :, D:2 * D] = dys
        in_copy(k).start()

    xs, dys = fill(0)
    recv[0, :, 0:D] = xs
    recv[0, :, D:2 * D] = dys

    slots_t = jnp.transpose(slots)
    gates_t = jnp.transpose(gates)
    for k in range(N):
        slot_col[k] = jnp.broadcast_to(slots_t[:, k:k + 1], (TOK, 128))
        gate_col[k] = jnp.broadcast_to(gates_t[:, k:k + 1], (TOK, 128))
    acc_y[...] = jnp.zeros_like(acc_y)
    acc_dx[...] = jnp.zeros_like(acc_dx)
    acc_dg[...] = jnp.zeros_like(acc_dg)

    w1_in.wait()
    w2_in.wait()

    @pl.loop(0, N // 2)
    def _(j):
        k0 = 2 * j
        k1 = k0 + 1

        @pl.when(j > 0)
        def _():
            in_copy(k0).wait_recv()

        in_copy(k1).wait_recv()
        xr = recv[pl.ds(k0, 2), :, 0:D].reshape(2 * CAP, D)
        dyr = recv[pl.ds(k0, 2), :, D:2 * D].reshape(2 * CAP, D)
        a = nn(xr, w1[...])
        dh = nt(dyr, w2[...])
        a2 = a * a
        t = jnp.tanh(a * (GELU_C + (GELU_C * GELU_A) * a2))
        half = 0.5 + 0.5 * t
        h = (a * half).astype(BF16)
        slope = half + (0.5 * a) * (1.0 - t * t) * (GELU_C + (3.0 * GELU_C * GELU_A) * a2)
        da = (dh * slope).astype(BF16)
        rows = pl.ds(pl.multiple_of(k0 * CAP, 2 * CAP), 2 * CAP)
        hid[rows, :] = h
        dpre[rows, :] = da
        ys[pl.ds(k0, 2)] = nn(h, w2[...]).astype(BF16).reshape(2, CAP, D)

        @pl.when(j > 0)
        def _():
            y_copy(k0).start()

        y_copy(k1).start()
        dxs[pl.ds(k0, 2)] = nt(da, w1[...]).astype(BF16).reshape(2, CAP, D)

    @pl.loop(1, N)
    def _(k):
        dx_copy(k).start()

    yr[0] = ys[0]
    dxr[0] = dxs[0]

    xt = recv[:, :, 0:D].reshape(N * CAP, D)
    dyt = recv[:, :, D:2 * D].reshape(N * CAP, D)

    @pl.loop(0, H // 256)
    def _(c):
        cols = pl.ds(pl.multiple_of(c * 256, 256), 256)
        gwi[:, cols] = tn(xt, dpre[:, cols])
        gwo[cols, :] = jnp.transpose(tn(dyt, hid[:, cols]))

    gwi_out = pltpu.make_async_copy(gwi, gwi_hbm, loc.at[2])
    gwo_out = pltpu.make_async_copy(gwo, gwo_hbm, loc.at[3])
    gwi_out.start()
    gwo_out.start()

    lane_f = lax.broadcasted_iota(jnp.int32, (TOK, CAP), 1).astype(F32)
    lane_i = lax.broadcasted_iota(jnp.int32, (TOK, 128), 1)

    @pl.loop(0, N)
    def _(k):
        @pl.when(k > 0)
        def _():
            y_copy(k).wait_recv()

        sel = jnp.where(slot_col[k] == lane_f, 1.0, 0.0).astype(BF16)
        zy = nn(sel, yr[k])
        gc = gate_col[k]
        acc_y[:, 0:128] += gc * zy[:, 0:128]
        acc_y[:, 128:256] += gc * zy[:, 128:256]
        dg = jnp.sum(zy * do_ref[...].astype(F32), axis=1, keepdims=True)
        acc_dg[...] += jnp.where(lane_i == k, dg, 0.0)

    y_ref[...] = acc_y[...].astype(BF16)
    gmat = jnp.concatenate([gates_t, jnp.zeros((TOK, 128 - N), F32)], axis=1)
    dgm = acc_dg[...]
    mean = jnp.sum(gmat * dgm, axis=1, keepdims=True)
    dl = (gmat * (dgm - mean)).astype(BF16)
    perm_r = lax.broadcasted_iota(jnp.int32, (128, N), 0)
    perm_c = lax.broadcasted_iota(jnp.int32, (128, N), 1)
    perm = jnp.where(jnp.bitwise_xor(perm_c, me) == perm_r, 1.0, 0.0).astype(BF16)
    d_log = nn(dl, perm).astype(BF16)
    gbuf[me] = tn(d_log, x_ref[...])

    def g_copy(k):
        return rcopy(gbuf.at[me], gbuf.at[me], g_s.at[k], g_r.at[k], k)

    @pl.loop(1, N)
    def _(k):
        g_copy(k).start()

    gate_part = nn(d_log, wg_ref[...])

    @pl.loop(0, N)
    def _(k):
        @pl.when(k > 0)
        def _():
            dx_copy(k).wait_recv()

        sel = jnp.where(slot_col[k] == lane_f, 1.0, 0.0).astype(BF16)
        acc_dx[...] += nn(sel, dxr[k])

    gx_ref[...] = (acc_dx[...] + gate_part).astype(BF16)

    @pl.loop(1, N)
    def _(k):
        pr = peer_of(me, k)
        rcopy(gbuf.at[pr], gbuf.at[pr], g_s.at[k], g_r.at[k], k).wait_recv()

    total = gbuf[0]
    for s in range(1, N):
        total = total + gbuf[s]
    gwg_ref[...] = total

    gwi_out.wait()
    gwo_out.wait()

    @pl.loop(1, N)
    def _(k):
        in_copy(k).wait_send()
        y_copy(k).wait_send()
        dx_copy(k).wait_send()
        g_copy(k).wait_send()


def local_block(tokens, grad_out, expert_ids, w_gate, w_in, w_out):
    vm = pl.BlockSpec(memory_space=pltpu.VMEM)
    anyspace = pl.BlockSpec(memory_space=pl.ANY)
    dma = pltpu.SemaphoreType.DMA
    y, gx, gwi, gwo, gwg = pl.pallas_call(
        kernel,
        out_shape=(
            jax.ShapeDtypeStruct((TOK, D), BF16),
            jax.ShapeDtypeStruct((TOK, D), BF16),
            jax.ShapeDtypeStruct((D, H), F32),
            jax.ShapeDtypeStruct((H, D), F32),
            jax.ShapeDtypeStruct((N, D), F32),
        ),
        in_specs=[vm, vm, vm, vm, anyspace, anyspace],
        out_specs=(vm, vm, anyspace, anyspace, vm),
        scratch_shapes=[
            pltpu.VMEM((D, H), BF16),
            pltpu.VMEM((H, D), BF16),
            pltpu.VMEM((N, CAP, 2 * D), BF16),
            pltpu.VMEM((N, CAP, 2 * D), BF16),
            pltpu.VMEM((N, CAP, D), BF16),
            pltpu.VMEM((N, CAP, D), BF16),
            pltpu.VMEM((N, CAP, D), BF16),
            pltpu.VMEM((N, CAP, D), BF16),
            pltpu.VMEM((N * CAP, H), BF16),
            pltpu.VMEM((N * CAP, H), BF16),
            pltpu.VMEM((D, H), F32),
            pltpu.VMEM((H, D), F32),
            pltpu.VMEM((N, TOK), F32),
            pltpu.VMEM((N, TOK), F32),
            pltpu.VMEM((N, TOK, 128), F32),
            pltpu.VMEM((N, TOK, 128), F32),
            pltpu.VMEM((TOK, D), F32),
            pltpu.VMEM((TOK, D), F32),
            pltpu.VMEM((TOK, 128), F32),
            pltpu.VMEM((N, N, D), F32),
            dma((N,)), dma((N,)), dma((N,)), dma((N,)), dma((N,)), dma((N,)), dma((N,)), dma((N,)),
            dma((4,)),
        ],
        compiler_params=pltpu.CompilerParams(collective_id=0, has_side_effects=True, vmem_limit_bytes=56 * 2 ** 20),
    )(tokens, grad_out, expert_ids.T, w_gate.T, w_in[0], w_out[0])
    return y, gx, gwi[None], gwo[None], gwg.T


def solution(mesh):
    return jax.shard_map(local_block, mesh=mesh, in_specs=(P('ep'), P('ep'), P('ep'), P(), P('ep'), P('ep')), out_specs=(P('ep'), P('ep'), P('ep'), P('ep'), P()), check_vma=False)
```

```python
import functools

import jax
import jax.numpy as jnp
from jax import lax
from jax.experimental import pallas as pl
from jax.experimental.pallas import tpu as pltpu
from jax.sharding import PartitionSpec as P

N = 16
CAP = 128
TOK = 512
D = 256
H = 1024
MESH = pl.DeviceIdType.MESH
F32 = jnp.float32
BF16 = jnp.bfloat16
GELU_C = 0.7978845608028654
GELU_A = 0.044715


def peer_of(me, k):
    out = me
    for bit in (1, 2, 4, 8):
        mine = (me // bit) % 2
        flip = (k // bit) % 2
        out = out + flip * bit * (1 - 2 * mine)
    return out


def nn(a, b):
    return lax.dot_general(a, b, (((1,), (0,)), ((), ())), preferred_element_type=F32)


def nt(a, b):
    return lax.dot_general(a, b, (((1,), (1,)), ((), ())), preferred_element_type=F32)


def tn(a, b):
    return lax.dot_general(a, b, (((0,), (0,)), ((), ())), preferred_element_type=F32)


def kernel(x_ref, do_ref, ids_ref, wg_ref, w1_hbm, w2_hbm,
           y_ref, gx_ref, gwi, gwo, gwg_ref,
           w1, w2, send, recv, ys, yr, dxs, dxr, hid, dpre,
           slot_row, gate_row, slot_col, gate_col, acc_y, acc_dx, acc_dg, gpart, grecv, gall,
           in_s, in_r, y_s, y_r, dx_s, dx_r, g_s, g_r, a_s, a_r, loc):
    me = lax.axis_index('ep')

    def rcopy(src, dst, s_sem, r_sem, k):
        return pltpu.make_async_remote_copy(src_ref=src, dst_ref=dst, send_sem=s_sem, recv_sem=r_sem, device_id=(peer_of(me, k),), device_id_type=MESH)

    def in_copy(k):
        return rcopy(send.at[k], recv.at[k], in_s.at[k], in_r.at[k], k)

    def y_copy(k):
        return rcopy(ys.at[k], yr.at[k], y_s.at[k], y_r.at[k], k)

    def dx_copy(k):
        return rcopy(dxs.at[k], dxr.at[k], dx_s.at[k], dx_r.at[k], k)

    barrier = pltpu.get_barrier_semaphore()

    @pl.loop(1, N)
    def _(k):
        pl.semaphore_signal(barrier, inc=1, device_id=(peer_of(me, k),), device_id_type=MESH)

    w1_in = pltpu.make_async_copy(w1_hbm, w1, loc.at[0])
    w2_in = pltpu.make_async_copy(w2_hbm, w2, loc.at[1])
    w1_in.start()
    w2_in.start()

    x = x_ref[...]
    logits = nt(wg_ref[...], x)
    id0 = ids_ref[0:1, :]
    id1 = ids_ref[1:2, :]
    exp_iota = lax.broadcasted_iota(jnp.int32, (N, TOK), 0)
    l0 = jnp.sum(jnp.where(exp_iota == id0, logits, 0.0), axis=0, keepdims=True)
    l1 = jnp.sum(jnp.where(exp_iota == id1, logits, 0.0), axis=0, keepdims=True)
    top = jnp.maximum(l0, l1)
    e0 = jnp.exp(l0 - top)
    e1 = jnp.exp(l1 - top)
    g0 = e0 / (e0 + e1)
    g1 = e1 / (e0 + e1)
    peer_iota = jnp.bitwise_xor(exp_iota, me)
    hot0 = peer_iota == id0
    hot1 = peer_iota == id1
    named = jnp.logical_or(hot0, hot1)
    row_i = lax.broadcasted_iota(jnp.int32, (TOK, TOK), 0)
    col_i = lax.broadcasted_iota(jnp.int32, (TOK, TOK), 1)
    before = jnp.where(row_i < col_i, 1.0, 0.0).astype(BF16)
    rank = nn(jnp.where(named, 1.0, 0.0).astype(BF16), before)
    slots = jnp.where(named, rank, -1.0)
    gates = jnp.where(hot0, g0, 0.0) + jnp.where(hot1, g1, 0.0)
    slot_row[...] = slots
    gate_row[...] = gates

    slot_iota = lax.broadcasted_iota(jnp.int32, (CAP, TOK), 0).astype(F32)

    def fill(k):
        hit = slot_iota == slot_row[pl.ds(k, 1), :]
        sel = jnp.where(hit, 1.0, 0.0).astype(BF16)
        g_slot = jnp.sum(jnp.where(hit, gate_row[pl.ds(k, 1), :], 0.0), axis=1, keepdims=True)
        return nn(sel, x_ref[...]).astype(BF16), (g_slot * nn(sel, do_ref[...])).astype(BF16)

    @pl.loop(1, N)
    def _(k):
        xs, dys = fill(k)
        send[k, :, 0:D] = xs
        send[k, :, D:2 * D] = dys

    pl.semaphore_wait(barrier, N - 1)

    @pl.loop(1, N)
    def _(k):
        in_copy(k).start()

    xs, dys = fill(0)
    recv[0, :, 0:D] = xs
    recv[0, :, D:2 * D] = dys

    slots_t = jnp.transpose(slots)
    gates_t = jnp.transpose(gates)
    for k in range(N):
        slot_col[k] = jnp.broadcast_to(slots_t[:, k:k + 1], (TOK, 128))
        gate_col[k] = jnp.broadcast_to(gates_t[:, k:k + 1], (TOK, 128))
    acc_y[...] = jnp.zeros_like(acc_y)
    acc_dx[...] = jnp.zeros_like(acc_dx)
    acc_dg[...] = jnp.zeros_like(acc_dg)

    w1_in.wait()
    w2_in.wait()

    @pl.loop(0, N // 2)
    def _(j):
        k0 = 2 * j
        k1 = k0 + 1

        @pl.when(j > 0)
        def _():
            in_copy(k0).wait_recv()

        in_copy(k1).wait_recv()
        xr = recv[pl.ds(k0, 2), :, 0:D].reshape(2 * CAP, D)
        dyr = recv[pl.ds(k0, 2), :, D:2 * D].reshape(2 * CAP, D)
        a = nn(xr, w1[...])
        dh = nt(dyr, w2[...])
        a2 = a * a
        t = jnp.tanh(a * (GELU_C + (GELU_C * GELU_A) * a2))
        half = 0.5 + 0.5 * t
        h = (a * half).astype(BF16)
        slope = half + (0.5 * a) * (1.0 - t * t) * (GELU_C + (3.0 * GELU_C * GELU_A) * a2)
        da = (dh * slope).astype(BF16)
        rows = pl.ds(pl.multiple_of(k0 * CAP, 2 * CAP), 2 * CAP)
        hid[rows, :] = h
        dpre[rows, :] = da
        ys[pl.ds(k0, 2)] = nn(h, w2[...]).astype(BF16).reshape(2, CAP, D)

        @pl.when(j > 0)
        def _():
            y_copy(k0).start()

        y_copy(k1).start()
        dxs[pl.ds(k0, 2)] = nt(da, w1[...]).astype(BF16).reshape(2, CAP, D)

    @pl.loop(1, N // 2)
    def _(j):
        dx_copy(2 * j).start()

    yr[0] = ys[0]
    dxr[0] = dxs[0]

    xt = recv[:, :, 0:D].reshape(N * CAP, D)
    dyt = recv[:, :, D:2 * D].reshape(N * CAP, D)

    @pl.loop(0, H // 256)
    def _(c):
        cols = pl.ds(pl.multiple_of(c * 256, 256), 256)
        gwi[:, cols] = tn(xt, dpre[:, cols])
        gwo[cols, :] = jnp.transpose(tn(dyt, hid[:, cols]))

    lane_f = lax.broadcasted_iota(jnp.int32, (TOK, CAP), 1).astype(F32)
    lane_i = lax.broadcasted_iota(jnp.int32, (TOK, 128), 1)

    @pl.loop(0, N)
    def _(k):
        @pl.when(k > 0)
        def _():
            y_copy(k).wait_recv()

        sel = jnp.where(slot_col[k] == lane_f, 1.0, 0.0).astype(BF16)
        zy = nn(sel, yr[k])
        gc = gate_col[k]
        acc_y[:, 0:128] += gc * zy[:, 0:128]
        acc_y[:, 128:256] += gc * zy[:, 128:256]
        dg = jnp.sum(zy * do_ref[...].astype(F32), axis=1, keepdims=True)
        acc_dg[...] += jnp.where(lane_i == k, dg, 0.0)

    y_ref[...] = acc_y[...].astype(BF16)
    gmat = jnp.concatenate([gates_t, jnp.zeros((TOK, 128 - N), F32)], axis=1)
    dgm = acc_dg[...]
    mean = jnp.sum(gmat * dgm, axis=1, keepdims=True)
    dl = (gmat * (dgm - mean)).astype(BF16)

    part = tn(dl, x_ref[...])
    for k in range(N):
        gpart[k] = part[k:k + 1, :]

    def part_copy(k):
        return rcopy(gpart.at[k], grecv.at[k], g_s.at[k], g_r.at[k], k)

    def sum_copy(k):
        return rcopy(gall.at[me], gall.at[me], a_s.at[k], a_r.at[k], k)

    @pl.loop(1, N)
    def _(k):
        part_copy(k).start()

    @pl.loop(0, N // 2)
    def _(j):
        dx_copy(2 * j + 1).start()

    perm_r = lax.broadcasted_iota(jnp.int32, (128, N), 0)
    perm_c = lax.broadcasted_iota(jnp.int32, (128, N), 1)
    perm = jnp.where(jnp.bitwise_xor(perm_c, me) == perm_r, 1.0, 0.0).astype(BF16)
    d_log = nn(dl, perm).astype(BF16)
    gate_part = nn(d_log, wg_ref[...])

    def add_dx(k):
        sel = jnp.where(slot_col[k] == lane_f, 1.0, 0.0).astype(BF16)
        acc_dx[...] += nn(sel, dxr[k])

    @pl.loop(0, N // 2)
    def _(j):
        @pl.when(j > 0)
        def _():
            dx_copy(2 * j).wait_recv()

        add_dx(2 * j)

    @pl.loop(1, N)
    def _(k):
        part_copy(k).wait_recv()

    total = gpart[0]
    for k in range(1, N):
        total = total + grecv[k]
    gall[me] = total

    @pl.loop(1, N)
    def _(k):
        sum_copy(k).start()

    @pl.loop(0, N // 2)
    def _(j):
        dx_copy(2 * j + 1).wait_recv()
        add_dx(2 * j + 1)

    gx_ref[...] = (acc_dx[...] + gate_part).astype(BF16)

    @pl.loop(1, N)
    def _(k):
        pr = peer_of(me, k)
        rcopy(gall.at[pr], gall.at[pr], a_s.at[k], a_r.at[k], k).wait_recv()

    for e in range(N):
        gwg_ref[e:e + 1, :] = gall[e]

    @pl.loop(1, N)
    def _(k):
        in_copy(k).wait_send()
        y_copy(k).wait_send()
        dx_copy(k).wait_send()
        part_copy(k).wait_send()
        sum_copy(k).wait_send()


def write_out(*refs):
    sem = refs[10]
    copies = [pltpu.make_async_copy(refs[i], refs[5 + i], sem.at[i]) for i in range(5)]
    for c in copies:
        c.start()
    for c in copies:
        c.wait()


def local_block(tokens, grad_out, expert_ids, w_gate, w_in, w_out):
    vm = pl.BlockSpec(memory_space=pltpu.VMEM)
    anyspace = pl.BlockSpec(memory_space=pl.ANY)
    dma = pltpu.SemaphoreType.DMA
    results = (((TOK, D), BF16), ((TOK, D), BF16), ((D, H), F32), ((H, D), F32), ((N, D), F32))
    raw = pl.pallas_call(
        kernel,
        out_shape=tuple(pltpu.VMEM(shape, dtype) for shape, dtype in results),
        in_specs=[vm, vm, vm, vm, anyspace, anyspace],
        out_specs=(vm,) * 5,
        scratch_shapes=[
            pltpu.VMEM((D, H), BF16),
            pltpu.VMEM((H, D), BF16),
            pltpu.VMEM((N, CAP, 2 * D), BF16),
            pltpu.VMEM((N, CAP, 2 * D), BF16),
            pltpu.VMEM((N, CAP, D), BF16),
            pltpu.VMEM((N, CAP, D), BF16),
            pltpu.VMEM((N, CAP, D), BF16),
            pltpu.VMEM((N, CAP, D), BF16),
            pltpu.VMEM((N * CAP, H), BF16),
            pltpu.VMEM((N * CAP, H), BF16),
            pltpu.VMEM((N, TOK), F32),
            pltpu.VMEM((N, TOK), F32),
            pltpu.VMEM((N, TOK, 128), F32),
            pltpu.VMEM((N, TOK, 128), F32),
            pltpu.VMEM((TOK, D), F32),
            pltpu.VMEM((TOK, D), F32),
            pltpu.VMEM((TOK, 128), F32),
            pltpu.VMEM((N, 1, D), F32),
            pltpu.VMEM((N, 1, D), F32),
            pltpu.VMEM((N, 1, D), F32),
            dma((N,)), dma((N,)), dma((N,)), dma((N,)), dma((N,)), dma((N,)), dma((N,)), dma((N,)), dma((N,)), dma((N,)),
            dma((2,)),
        ],
        compiler_params=pltpu.CompilerParams(collective_id=0, has_side_effects=True, vmem_limit_bytes=56 * 2 ** 20),
    )(tokens, grad_out, expert_ids.T, w_gate.T, w_in[0], w_out[0])
    raw = [pltpu.with_memory_space_constraint(r, pltpu.VMEM) for r in raw]
    y, gx, gwi, gwo, gwg = pl.pallas_call(
        write_out,
        out_shape=tuple(jax.ShapeDtypeStruct(shape, dtype) for shape, dtype in results),
        in_specs=[vm] * 5,
        out_specs=(anyspace,) * 5,
        scratch_shapes=[dma((5,))],
    )(*raw)
    return y, gx, gwi[None], gwo[None], gwg.T


def solution(mesh):
    return jax.shard_map(local_block, mesh=mesh, in_specs=(P('ep'), P('ep'), P('ep'), P(), P('ep'), P('ep')), out_specs=(P('ep'), P('ep'), P('ep'), P('ep'), P()), check_vma=False)
```

```python
import functools

import jax
import jax.numpy as jnp
from jax import lax
from jax.experimental import pallas as pl
from jax.experimental.pallas import tpu as pltpu
from jax.sharding import PartitionSpec as P

N = 16
CHIPS = N // 2
STEPS = CHIPS // 2
CAP = 128
BASE = 64
TOK = 512
D = 256
H = 1024
MESH = pl.DeviceIdType.MESH
F32 = jnp.float32
BF16 = jnp.bfloat16
GELU_C = 0.7978845608028654
GELU_A = 0.044715


def hops(me):
    return [bit * (1 - 2 * lax.rem(lax.div(me, bit), 2)) for bit in (1, 2, 4, 8)]


def peer_of(me, flips, k):
    out = me
    for i, bit in enumerate((1, 2, 4, 8)):
        if isinstance(k, int):
            out = out + flips[i] * ((k // bit) % 2) if (k // bit) % 2 else out
        else:
            out = out + flips[i] * lax.rem(lax.div(k, bit), 2)
    return out


def nn(a, b):
    return lax.dot_general(a, b, (((1,), (0,)), ((), ())), preferred_element_type=F32)


def nt(a, b):
    return lax.dot_general(a, b, (((1,), (1,)), ((), ())), preferred_element_type=F32)


def tn(a, b):
    return lax.dot_general(a, b, (((0,), (0,)), ((), ())), preferred_element_type=F32)


def chips_of(q):
    a = (7 * q - q * q) // 2 if isinstance(q, int) else lax.div(7 * q - q * q, 2)
    return a, CHIPS - 1 - a


def remote(at, src, dst, s_sem, r_sem, k):
    return pltpu.make_async_remote_copy(src_ref=src, dst_ref=dst, send_sem=s_sem, recv_sem=r_sem, device_id=(peer_of(*at, k),), device_id_type=MESH)


def greet(me, flips):
    barrier = pltpu.get_barrier_semaphore()

    for k in range(1, N):
        pl.semaphore_signal(barrier, inc=1, device_id=(peer_of(me, flips, k),), device_id_type=MESH)

    return barrier


def block(shared, x_hbm, ids_hbm, wg_hbm, do_hbm, w1_hbm, w2_hbm,
          y_ref, gx_ref, gwi, gwo, gwg_ref, full,
          x_ref, ids_ref, wg_ref, do_ref, w1, w2, slot_row, gate_row, tile, own,
          picked, send, sendo, recv, xt, dyt, ys, yr, dxs, dxr, omy, omd, yo, dxo, hid, dpre,
          slot_col, gate_col, acc_y, acc_dx, acc_dg, gpart, grecv, gall,
          in_s, in_r, io_s, io_r, fw_s, fw_r, y_s, y_r, yo_s, yo_r, dx_s, dx_r, do_s, do_r,
          my_s, my_r, md_s, md_r, g_s, g_r, a_s, a_r, f_s, f_r, loc):
    me = lax.axis_index('ep')
    rows = BASE if shared else CAP
    head = pl.ds(0, rows)
    tail = pl.ds(BASE, BASE)
    here = (me, hops(me))
    barrier = greet(*here)
    pairs = ((x_hbm, x_ref), (ids_hbm, ids_ref), (wg_hbm, wg_ref), (do_hbm, do_ref), (w1_hbm, w1), (w2_hbm, w2))
    loads = [pltpu.make_async_copy(a, b, loc.at[i]) for i, (a, b) in enumerate(pairs)]
    for c in loads:
        c.start()
    def in_copy(k):
        return remote(here, send.at[k], recv.at[k, head], in_s.at[k], in_r.at[k], k)

    def in_over(j):
        return remote(here, sendo.at[j], recv.at[2 * j, tail], io_s.at[j], io_r.at[j], 2 * j)

    def pass_on(j):
        return remote(here, recv.at[2 * j, tail], recv.at[2 * j + 1, tail], fw_s.at[j], fw_r.at[j], 1)

    def y_copy(k):
        return remote(here, ys.at[k, head], yr.at[k, head], y_s.at[k], y_r.at[k], k)

    def y_over(j):
        return remote(here, yo.at[j], yr.at[2 * j, tail], yo_s.at[j], yo_r.at[j], 2 * j)

    def y_merge(j):
        return remote(here, ys.at[2 * j + 1, tail], omy.at[j], my_s.at[j], my_r.at[j], 1)

    def dx_copy(k):
        return remote(here, dxs.at[k, head], dxr.at[k, head], dx_s.at[k], dx_r.at[k], k)

    def dx_over(j):
        return remote(here, dxo.at[j], dxr.at[2 * j, tail], do_s.at[j], do_r.at[j], 2 * j)

    def dx_merge(j):
        return remote(here, dxs.at[2 * j + 1, tail], omd.at[j], md_s.at[j], md_r.at[j], 1)

    def flag_copy(k):
        return remote(here, tile.at[k], own.at[k], f_s.at[k], f_r.at[k], k)

    for c in loads[0:3]:
        c.wait()
    id0 = ids_ref[0:1, :]
    id1 = ids_ref[1:2, :]
    exp_iota = lax.broadcasted_iota(jnp.int32, (N, TOK), 0)
    peer_iota = jnp.bitwise_xor(exp_iota, me)
    hot0 = peer_iota == id0
    hot1 = peer_iota == id1
    named = jnp.where(jnp.logical_or(hot0, hot1), 1.0, 0.0)
    row_i = lax.broadcasted_iota(jnp.int32, (TOK, TOK), 0)
    col_i = lax.broadcasted_iota(jnp.int32, (TOK, TOK), 1)
    before = jnp.where(row_i < col_i, 1.0, 0.0).astype(BF16)
    rank = nn(named.astype(BF16), before)
    slot_row[...] = jnp.where(named > 0.5, rank, -1.0)
    logits = nt(wg_ref[...], x_ref[...])
    l0 = jnp.sum(jnp.where(exp_iota == id0, logits, 0.0), axis=0, keepdims=True)
    l1 = jnp.sum(jnp.where(exp_iota == id1, logits, 0.0), axis=0, keepdims=True)
    top = jnp.maximum(l0, l1)
    e0 = jnp.exp(l0 - top)
    e1 = jnp.exp(l1 - top)
    g0 = e0 / (e0 + e1)
    g1 = e1 / (e0 + e1)
    gate_row[...] = jnp.where(hot0, g0, 0.0) + jnp.where(hot1, g1, 0.0)
    if shared:
        count = jnp.sum(named, axis=1, keepdims=True)
        over = jnp.broadcast_to(jnp.where(count > float(BASE), 1.0, 0.0), (N, 128))
        even = lax.rem(lax.broadcasted_iota(jnp.int32, (N, 128), 0), 2) == 0
        both = jnp.max(jnp.where(even, over * pltpu.roll(over, N - 1, 0), 0.0), axis=0, keepdims=True)
        left = lax.broadcasted_iota(jnp.int32, (1, 128), 1) < 64
        for k in range(N):
            tile[k] = jnp.where(left, over[k:k + 1, :], both)
        own[0] = tile[0]
    loads[3].wait()

    slot_iota = lax.broadcasted_iota(jnp.int32, (rows, TOK), 0).astype(F32)

    def fill_step(q):
        blocks = []
        for j in chips_of(q):
            for k in (2 * j, 2 * j + 1):
                hit = slot_iota == slot_row[pl.ds(k, 1), :]
                blocks.append((send, k, hit, jnp.where(hit, gate_row[pl.ds(k, 1), :], 0.0)))
            if shared:
                hit0 = slot_iota + float(BASE) == slot_row[pl.ds(2 * j, 1), :]
                hit1 = slot_iota + float(BASE) == slot_row[pl.ds(2 * j + 1, 1), :]
                gate = jnp.where(hit0, gate_row[pl.ds(2 * j, 1), :], 0.0) + jnp.where(hit1, gate_row[pl.ds(2 * j + 1, 1), :], 0.0)
                blocks.append((sendo, j, jnp.logical_or(hit0, hit1), gate))
        for i, (_, _, hit, _) in enumerate(blocks):
            picked[i * rows:(i + 1) * rows, :] = jnp.where(hit, 1.0, 0.0).astype(BF16)
        sel = picked[0:len(blocks) * rows, :]
        xs = nn(sel, x_ref[...]).astype(BF16)
        dys = nn(sel, do_ref[...])
        for i, (to, at, _, gate) in enumerate(blocks):
            to[at, :, 0:D] = xs[i * rows:(i + 1) * rows]
            to[at, :, D:2 * D] = (jnp.sum(gate, axis=1, keepdims=True) * dys[i * rows:(i + 1) * rows]).astype(BF16)

    def send_chip(j):
        if shared:
            in_over(j).start()
        in_copy(2 * j).start()
        in_copy(2 * j + 1).start()

    fill_step(0)
    recv[0, 0:rows, :] = send[0]
    if shared:
        recv[0, BASE:2 * BASE, :] = sendo[0]

    @pl.loop(1, STEPS)
    def _(q):
        fill_step(q)

    pl.semaphore_wait(barrier, N - 1)
    if shared:
        @pl.loop(1, N)
        def _(k):
            flag_copy(k).start()

        pass_on(0).start()
    in_copy(1).start()
    send_chip(CHIPS - 1)

    @pl.loop(1, STEPS)
    def _(q):
        for j in chips_of(q):
            send_chip(j)

    slots_t = jnp.transpose(slot_row[...])
    gates_t = jnp.transpose(gate_row[...])
    for k in range(N):
        slot_col[k] = jnp.broadcast_to(slots_t[:, k:k + 1], (TOK, 128))
        gate_col[k] = jnp.broadcast_to(gates_t[:, k:k + 1], (TOK, 128))
    acc_y[...] = jnp.zeros_like(acc_y)
    acc_dx[...] = jnp.zeros_like(acc_dx)
    acc_dg[...] = jnp.zeros_like(acc_dg)

    def merge(j):
        y_merge(j).wait_recv()
        dx_merge(j).wait_recv()
        yo[j] = ys[2 * j, BASE:2 * BASE, :] + omy[j]
        dxo[j] = dxs[2 * j, BASE:2 * BASE, :] + omd[j]

    def expert(q, part, ks):
        at = pl.ds(pl.multiple_of(q * 4 * CAP + part * 2 * CAP, 2 * CAP), 2 * CAP)
        for i, k in enumerate(ks):
            to = pl.ds(pl.multiple_of(q * 4 * CAP + part * 2 * CAP + i * BASE, BASE), BASE)
            from_rows = slice(part * BASE, (part + 1) * BASE)
            xs = recv[k, from_rows, 0:D]
            dys = recv[k, from_rows, D:2 * D]
            if shared and part == 1:
                mine = own[pl.ds(k, 1), 0:1, 0:1].reshape(1, 1).astype(BF16)
                xs = xs * mine
                dys = dys * mine
            xt[to, :] = xs
            dyt[to, :] = dys
        a = nn(xt[at, :], w1[...])
        dh = nt(dyt[at, :], w2[...])
        a2 = a * a
        t = jnp.tanh(a * (GELU_C + (GELU_C * GELU_A) * a2))
        half = 0.5 + 0.5 * t
        h = (a * half).astype(BF16)
        slope = half + (0.5 * a) * (1.0 - t * t) * (GELU_C + (3.0 * GELU_C * GELU_A) * a2)
        da = (dh * slope).astype(BF16)
        hid[at, :] = h
        dpre[at, :] = da
        y = nn(h, w2[...]).astype(BF16)
        dx = nt(da, w1[...]).astype(BF16)
        for i, k in enumerate(ks):
            ys[k, part * BASE:(part + 1) * BASE, :] = y[i * BASE:(i + 1) * BASE]
            dxs[k, part * BASE:(part + 1) * BASE, :] = dx[i * BASE:(i + 1) * BASE]

    for c in loads[4:]:
        c.wait()
    if shared:
        @pl.loop(1, N)
        def _(k):
            flag_copy(k).wait_recv()

    if shared:
        seen = own[0]
        for k in range(1, N):
            seen = seen + own[k]
        full[...] = jnp.broadcast_to(seen, (8, 128))
    else:
        full[...] = jnp.zeros_like(full)

    @pl.loop(0, STEPS)
    def _(q):
        ja, jb = chips_of(q)
        ks = (2 * ja, 2 * ja + 1, 2 * jb, 2 * jb + 1)

        if shared:
            @pl.when(q > 0)
            def _():
                in_over(ja).wait_recv()
                pass_on(ja).start()

            in_over(jb).wait_recv()
            pass_on(jb).start()

        @pl.when(q > 0)
        def _():
            in_copy(ks[0]).wait_recv()

        for k in ks[1:]:
            in_copy(k).wait_recv()
        expert(q, 0, ks)
        if not shared:
            expert(q, 1, ks)

        @pl.when(q > 0)
        def _():
            y_copy(ks[0]).start()

        for k in ks[1:]:
            y_copy(k).start()
        if shared:
            @pl.when(q > 0)
            def _():
                for j in chips_of(q - 1):
                    merge(j)

                @pl.when(q > 1)
                def _():
                    y_over(chips_of(q - 1)[0]).start()

                y_over(chips_of(q - 1)[1]).start()

            for j in (ja, jb):
                pass_on(j).wait_recv()
            expert(q, 1, ks)
            for j in (ja, jb):
                y_merge(j).start()
                dx_merge(j).start()

    if shared:
        for j in chips_of(STEPS - 1):
            merge(j)
            y_over(j).start()

    def send_dx(q):
        for j in chips_of(q):
            def even(j=j):
                dx_copy(2 * j).start()
                if shared:
                    dx_over(j).start()

            if isinstance(j, int):
                even()
            else:
                pl.when(j > 0)(even)

            dx_copy(2 * j + 1).start()

    @pl.loop(0, STEPS // 2)
    def _(q):
        send_dx(q)

    yr[0, 0:rows, :] = ys[0, 0:rows, :]
    dxr[0, 0:rows, :] = dxs[0, 0:rows, :]
    if shared:
        yr[0, BASE:2 * BASE, :] = yo[0]
        dxr[0, BASE:2 * BASE, :] = dxo[0]

    lane_f = lax.broadcasted_iota(jnp.int32, (TOK, CAP), 1).astype(F32)
    lane_i = lax.broadcasted_iota(jnp.int32, (TOK, 128), 1)

    def picks(k):
        return jnp.where(slot_col[k] == lane_f, 1.0, 0.0).astype(BF16)

    @pl.loop(0, CHIPS)
    def _(p):
        ja, jb = chips_of(lax.div(p, 2))
        j = ja + lax.rem(p, 2) * (jb - ja)

        @pl.when(j > 0)
        def _():
            y_copy(2 * j).wait_recv()
            if shared:
                y_over(j).wait_recv()

        y_copy(2 * j + 1).wait_recv()
        if shared:
            yr[2 * j + 1, BASE:2 * BASE, :] = yr[2 * j, BASE:2 * BASE, :]
        for c in range(2):
            k = 2 * j + c
            zy = nn(picks(k), yr[k])
            gc = gate_col[k]
            acc_y[:, 0:128] += gc * zy[:, 0:128]
            acc_y[:, 128:256] += gc * zy[:, 128:256]
            dg = jnp.sum(zy * do_ref[...].astype(F32), axis=1, keepdims=True)
            acc_dg[...] += jnp.where(lane_i == k, dg, 0.0)

    gmat = jnp.concatenate([gates_t, jnp.zeros((TOK, 128 - N), F32)], axis=1)
    dgm = acc_dg[...]
    mean = jnp.sum(gmat * dgm, axis=1, keepdims=True)
    dl = (gmat * (dgm - mean)).astype(BF16)

    part = tn(dl, x_ref[...])
    for k in range(N):
        gpart[k] = part[k:k + 1, :]

    def part_copy(k):
        return remote(here, gpart.at[k], grecv.at[k], g_s.at[k], g_r.at[k], k)

    def sum_copy(k):
        return remote(here, gall.at[me], gall.at[me], a_s.at[k], a_r.at[k], k)

    @pl.loop(1, N)
    def _(k):
        part_copy(k).start()

    send_dx(2)
    send_dx(3)

    @pl.loop(0, H // 256)
    def _(c):
        cols = pl.ds(pl.multiple_of(c * 256, 256), 256)
        gwi[:, cols] = tn(xt[...], dpre[:, cols])

    @pl.loop(1, N)
    def _(k):
        part_copy(k).wait_recv()

    total = gpart[0]
    for k in range(1, N):
        total = total + grecv[k]
    gall[me] = total

    @pl.loop(1, N)
    def _(k):
        sum_copy(k).start()

    @pl.loop(0, H // 256)
    def _(c):
        cols = pl.ds(pl.multiple_of(c * 256, 256), 256)
        gwo[cols, :] = jnp.transpose(tn(dyt[...], hid[:, cols]))

    y_ref[...] = acc_y[...].astype(BF16)
    perm_r = lax.broadcasted_iota(jnp.int32, (128, N), 0)
    perm_c = lax.broadcasted_iota(jnp.int32, (128, N), 1)
    perm = jnp.where(jnp.bitwise_xor(perm_c, me) == perm_r, 1.0, 0.0).astype(BF16)
    d_log = nn(dl, perm).astype(BF16)
    gate_part = nn(d_log, wg_ref[...])

    @pl.loop(0, CHIPS)
    def _(p):
        ja, jb = chips_of(lax.div(p, 2))
        j = ja + lax.rem(p, 2) * (jb - ja)

        @pl.when(j > 0)
        def _():
            dx_copy(2 * j).wait_recv()
            if shared:
                dx_over(j).wait_recv()

        dx_copy(2 * j + 1).wait_recv()
        if shared:
            dxr[2 * j + 1, BASE:2 * BASE, :] = dxr[2 * j, BASE:2 * BASE, :]
        sel = jnp.concatenate([picks(2 * j), picks(2 * j + 1)], axis=1)
        acc_dx[...] += nn(sel, dxr[pl.ds(2 * j, 2)].reshape(2 * CAP, D))

    gx_ref[...] = (acc_dx[...] + gate_part).astype(BF16)

    @pl.loop(1, N)
    def _(k):
        pr = peer_of(*here, k)
        remote(here, gall.at[pr], gall.at[pr], a_s.at[k], a_r.at[k], k).wait_recv()

    for e in range(N):
        gwg_ref[e:e + 1, :] = gall[e]

    @pl.loop(1, N)
    def _(k):
        in_copy(k).wait_send()
        y_copy(k).wait_send()
        dx_copy(k).wait_send()
        part_copy(k).wait_send()
        sum_copy(k).wait_send()

    if shared:
        @pl.loop(1, N)
        def _(k):
            flag_copy(k).wait_send()

        @pl.loop(0, CHIPS)
        def _(j):
            pass_on(j).wait_send()
            y_merge(j).wait_send()
            dx_merge(j).wait_send()

            @pl.when(j > 0)
            def _():
                in_over(j).wait_send()
                y_over(j).wait_send()
                dx_over(j).wait_send()


def write_out(*refs):
    sem = refs[10]
    copies = [pltpu.make_async_copy(refs[i], refs[5 + i], sem.at[i]) for i in range(5)]
    for c in copies:
        c.start()
    for c in copies:
        c.wait()


RESULTS = (((TOK, D), BF16), ((TOK, D), BF16), ((D, H), F32), ((H, D), F32), ((N, D), F32))


def run_block(shared, *args):
    vm = pl.BlockSpec(memory_space=pltpu.VMEM)
    anyspace = pl.BlockSpec(memory_space=pl.ANY)
    dma = pltpu.SemaphoreType.DMA
    rows = BASE if shared else CAP
    over = BASE if shared else 8
    return pl.pallas_call(
        functools.partial(block, shared),
        out_shape=tuple(pltpu.VMEM(shape, dtype) for shape, dtype in RESULTS + (((8, 128), F32),)),
        in_specs=[anyspace] * 6,
        out_specs=(vm,) * 6,
        scratch_shapes=[
            pltpu.VMEM((TOK, D), BF16),
            pltpu.VMEM((2, TOK), jnp.int32),
            pltpu.VMEM((N, D), BF16),
            pltpu.VMEM((TOK, D), BF16),
            pltpu.VMEM((D, H), BF16),
            pltpu.VMEM((H, D), BF16),
            pltpu.VMEM((N, TOK), F32),
            pltpu.VMEM((N, TOK), F32),
            pltpu.VMEM((N, 1, 128), F32),
            pltpu.VMEM((N, 1, 128), F32),
            pltpu.VMEM((4 * CAP, TOK), BF16),
            pltpu.VMEM((N, rows, 2 * D), BF16),
            pltpu.VMEM((CHIPS, over, 2 * D), BF16),
            pltpu.VMEM((N, CAP, 2 * D), BF16),
            pltpu.VMEM((N * CAP, D), BF16),
            pltpu.VMEM((N * CAP, D), BF16),
            *[pltpu.VMEM((N, CAP, D), BF16)] * 4,
            *[pltpu.VMEM((CHIPS, over, D), BF16)] * 4,
            pltpu.VMEM((N * CAP, H), BF16),
            pltpu.VMEM((N * CAP, H), BF16),
            pltpu.VMEM((N, TOK, 128), F32),
            pltpu.VMEM((N, TOK, 128), F32),
            pltpu.VMEM((TOK, D), F32),
            pltpu.VMEM((TOK, D), F32),
            pltpu.VMEM((TOK, 128), F32),
            *[pltpu.VMEM((N, 1, D), F32)] * 3,
            *[dma((N,))] * 2,
            *[dma((CHIPS,))] * 4,
            *[dma((N,))] * 2,
            *[dma((CHIPS,))] * 2,
            *[dma((N,))] * 2,
            *[dma((CHIPS,))] * 6,
            *[dma((N,))] * 6,
            dma((6,)),
        ],
        compiler_params=pltpu.CompilerParams(collective_id=0 if shared else 1, has_side_effects=True, vmem_limit_bytes=56 * 2 ** 20),
    )(*args)


def finish(*raw):
    vm = pl.BlockSpec(memory_space=pltpu.VMEM)
    anyspace = pl.BlockSpec(memory_space=pl.ANY)
    return pl.pallas_call(
        write_out,
        out_shape=tuple(jax.ShapeDtypeStruct(shape, dtype) for shape, dtype in RESULTS),
        in_specs=[vm] * 5,
        out_specs=(anyspace,) * 5,
        scratch_shapes=[pltpu.SemaphoreType.DMA((5,))],
        compiler_params=pltpu.CompilerParams(vmem_limit_bytes=2 ** 20),
    )(*[pltpu.with_memory_space_constraint(r, pltpu.VMEM) for r in raw])


def local_block(tokens, grad_out, expert_ids, w_gate, w_in, w_out):
    args = (tokens, expert_ids.T, w_gate.T, grad_out, w_in[0], w_out[0])
    *raw, full = run_block(True, *args)
    raw = [pltpu.with_memory_space_constraint(r, pltpu.VMEM) for r in raw]
    y, gx, gwi, gwo, gwg = lax.cond(
        full[0, 127] > 0.5,
        lambda raw, args: finish(*run_block(False, *args)[:5]),
        lambda raw, args: finish(*raw),
        raw, args)
    return y, gx, gwi[None], gwo[None], gwg.T


def solution(mesh):
    return jax.shard_map(local_block, mesh=mesh, in_specs=(P('ep'), P('ep'), P('ep'), P(), P('ep'), P('ep')), out_specs=(P('ep'), P('ep'), P('ep'), P('ep'), P()), check_vma=False)
```

```python
import functools

import jax
import jax.numpy as jnp
from jax import lax
from jax.experimental import pallas as pl
from jax.experimental.pallas import tpu as pltpu
from jax.sharding import PartitionSpec as P

N = 16
CHIPS = N // 2
STEPS = CHIPS // 2
CAP = 128
BASE = 64
TOK = 512
D = 256
H = 1024
MESH = pl.DeviceIdType.MESH
F32 = jnp.float32
BF16 = jnp.bfloat16
GELU_C = 0.7978845608028654
GELU_A = 0.044715


def hops(me):
    return [bit * (1 - 2 * lax.rem(lax.div(me, bit), 2)) for bit in (1, 2, 4, 8)]


def peer_of(me, flips, k):
    out = me
    for i, bit in enumerate((1, 2, 4, 8)):
        if isinstance(k, int):
            out = out + flips[i] * ((k // bit) % 2) if (k // bit) % 2 else out
        else:
            out = out + flips[i] * lax.rem(lax.div(k, bit), 2)
    return out


def nn(a, b):
    return lax.dot_general(a, b, (((1,), (0,)), ((), ())), preferred_element_type=F32)


def nt(a, b):
    return lax.dot_general(a, b, (((1,), (1,)), ((), ())), preferred_element_type=F32)


def tn(a, b):
    return lax.dot_general(a, b, (((0,), (0,)), ((), ())), preferred_element_type=F32)


def chips_of(q):
    a = (7 * q - q * q) // 2 if isinstance(q, int) else lax.div(7 * q - q * q, 2)
    return a, CHIPS - 1 - a


def remote(at, src, dst, s_sem, r_sem, k):
    return pltpu.make_async_remote_copy(src_ref=src, dst_ref=dst, send_sem=s_sem, recv_sem=r_sem, device_id=(peer_of(*at, k),), device_id_type=MESH)


def greet(me, flips):
    barrier = pltpu.get_barrier_semaphore()

    for k in range(1, N):
        pl.semaphore_signal(barrier, inc=1, device_id=(peer_of(me, flips, k),), device_id_type=MESH)

    return barrier


def block(shared, x_hbm, ids_hbm, wg_hbm, do_hbm, w1_hbm, w2_hbm,
          y_ref, gx_ref, gwi, gwo, gwg_ref, full,
          x_ref, ids_ref, wg_ref, do_ref, w1, w2, slot_row, gate_row, tile, own,
          picked, send, sendo, recv, xt, dyt, ys, yr, dxs, dxr, omy, omd, yo, dxo, hid, dpre,
          slot_col, gate_col, acc_y, acc_dx, acc_dg, gpart, grecv, gall,
          in_s, in_r, io_s, io_r, fw_s, fw_r, y_s, y_r, yo_s, yo_r, dx_s, dx_r, do_s, do_r,
          my_s, my_r, md_s, md_r, g_s, g_r, a_s, a_r, f_s, f_r, loc):
    me = lax.axis_index('ep')
    rows = BASE if shared else CAP
    head = pl.ds(0, rows)
    tail = pl.ds(BASE, BASE)
    here = (me, hops(me))
    barrier = greet(*here)
    pairs = ((x_hbm, x_ref), (ids_hbm, ids_ref), (wg_hbm, wg_ref), (do_hbm, do_ref), (w1_hbm, w1), (w2_hbm, w2))
    loads = [pltpu.make_async_copy(a, b, loc.at[i]) for i, (a, b) in enumerate(pairs)]
    for c in loads:
        c.start()
    def in_copy(k):
        return remote(here, send.at[k], recv.at[k, head], in_s.at[k], in_r.at[k], k)

    def in_over(j):
        return remote(here, sendo.at[j], recv.at[2 * j, tail], io_s.at[j], io_r.at[j], 2 * j)

    def pass_on(j):
        return remote(here, recv.at[2 * j, tail], recv.at[2 * j + 1, tail], fw_s.at[j], fw_r.at[j], 1)

    def y_copy(k):
        return remote(here, ys.at[k, head], yr.at[k, head], y_s.at[k], y_r.at[k], k)

    def y_over(j):
        return remote(here, yo.at[j], yr.at[2 * j, tail], yo_s.at[j], yo_r.at[j], 2 * j)

    def y_merge(j):
        return remote(here, ys.at[2 * j + 1, tail], omy.at[j], my_s.at[j], my_r.at[j], 1)

    def dx_copy(k):
        return remote(here, dxs.at[k, head], dxr.at[k, head], dx_s.at[k], dx_r.at[k], k)

    def dx_over(j):
        return remote(here, dxo.at[j], dxr.at[2 * j, tail], do_s.at[j], do_r.at[j], 2 * j)

    def dx_merge(j):
        return remote(here, dxs.at[2 * j + 1, tail], omd.at[j], md_s.at[j], md_r.at[j], 1)

    def flag_copy(k):
        return remote(here, tile.at[k], own.at[k], f_s.at[k], f_r.at[k], k)

    for c in loads[0:3]:
        c.wait()
    id0 = ids_ref[0:1, :]
    id1 = ids_ref[1:2, :]
    exp_iota = lax.broadcasted_iota(jnp.int32, (N, TOK), 0)
    peer_iota = jnp.bitwise_xor(exp_iota, me)
    hot0 = peer_iota == id0
    hot1 = peer_iota == id1
    named = jnp.where(jnp.logical_or(hot0, hot1), 1.0, 0.0)
    row_i = lax.broadcasted_iota(jnp.int32, (TOK, TOK), 0)
    col_i = lax.broadcasted_iota(jnp.int32, (TOK, TOK), 1)
    before = jnp.where(row_i < col_i, 1.0, 0.0).astype(BF16)
    rank = nn(named.astype(BF16), before)
    slot_row[...] = jnp.where(named > 0.5, rank, -1.0)
    logits = nt(wg_ref[...], x_ref[...])
    l0 = jnp.sum(jnp.where(exp_iota == id0, logits, 0.0), axis=0, keepdims=True)
    l1 = jnp.sum(jnp.where(exp_iota == id1, logits, 0.0), axis=0, keepdims=True)
    top = jnp.maximum(l0, l1)
    e0 = jnp.exp(l0 - top)
    e1 = jnp.exp(l1 - top)
    g0 = e0 / (e0 + e1)
    g1 = e1 / (e0 + e1)
    gate_row[...] = jnp.where(hot0, g0, 0.0) + jnp.where(hot1, g1, 0.0)
    if shared:
        count = jnp.sum(named, axis=1, keepdims=True)
        over = jnp.broadcast_to(jnp.where(count > float(BASE), 1.0, 0.0), (N, 128))
        even = lax.rem(lax.broadcasted_iota(jnp.int32, (N, 128), 0), 2) == 0
        both = jnp.max(jnp.where(even, over * pltpu.roll(over, N - 1, 0), 0.0), axis=0, keepdims=True)
        left = lax.broadcasted_iota(jnp.int32, (1, 128), 1) < 64
        for k in range(N):
            tile[k] = jnp.where(left, over[k:k + 1, :], both)
        own[0] = tile[0]
    loads[3].wait()

    slot_iota = lax.broadcasted_iota(jnp.int32, (rows, TOK), 0).astype(F32)

    def fill_step(q):
        blocks = []
        for j in chips_of(q):
            for k in (2 * j, 2 * j + 1):
                hit = slot_iota == slot_row[pl.ds(k, 1), :]
                blocks.append((send, k, hit, jnp.where(hit, gate_row[pl.ds(k, 1), :], 0.0)))
            if shared:
                hit0 = slot_iota + float(BASE) == slot_row[pl.ds(2 * j, 1), :]
                hit1 = slot_iota + float(BASE) == slot_row[pl.ds(2 * j + 1, 1), :]
                gate = jnp.where(hit0, gate_row[pl.ds(2 * j, 1), :], 0.0) + jnp.where(hit1, gate_row[pl.ds(2 * j + 1, 1), :], 0.0)
                blocks.append((sendo, j, jnp.logical_or(hit0, hit1), gate))
        for i, (_, _, hit, _) in enumerate(blocks):
            picked[i * rows:(i + 1) * rows, :] = jnp.where(hit, 1.0, 0.0).astype(BF16)
        sel = picked[0:len(blocks) * rows, :]
        xs = nn(sel, x_ref[...]).astype(BF16)
        dys = nn(sel, do_ref[...])
        for i, (to, at, _, gate) in enumerate(blocks):
            to[at, :, 0:D] = xs[i * rows:(i + 1) * rows]
            to[at, :, D:2 * D] = (jnp.sum(gate, axis=1, keepdims=True) * dys[i * rows:(i + 1) * rows]).astype(BF16)

    def send_chip(j):
        if shared:
            in_over(j).start()
        in_copy(2 * j).start()
        in_copy(2 * j + 1).start()

    fill_step(0)
    recv[0, 0:rows, :] = send[0]
    if shared:
        recv[0, BASE:2 * BASE, :] = sendo[0]

    @pl.loop(1, STEPS)
    def _(q):
        fill_step(q)

    pl.semaphore_wait(barrier, N - 1)
    if shared:
        @pl.loop(1, N)
        def _(k):
            flag_copy(k).start()

        pass_on(0).start()
    in_copy(1).start()
    send_chip(CHIPS - 1)

    @pl.loop(1, STEPS)
    def _(q):
        for j in chips_of(q):
            send_chip(j)

    slots_t = jnp.transpose(slot_row[...])
    gates_t = jnp.transpose(gate_row[...])
    for k in range(N):
        slot_col[k] = jnp.broadcast_to(slots_t[:, k:k + 1], (TOK, 128))
        gate_col[k] = jnp.broadcast_to(gates_t[:, k:k + 1], (TOK, 128))
    acc_y[...] = jnp.zeros_like(acc_y)
    acc_dx[...] = jnp.zeros_like(acc_dx)
    acc_dg[...] = jnp.zeros_like(acc_dg)

    def merge(j):
        y_merge(j).wait_recv()
        dx_merge(j).wait_recv()
        yo[j] = ys[2 * j, BASE:2 * BASE, :] + omy[j]
        dxo[j] = dxs[2 * j, BASE:2 * BASE, :] + omd[j]

    def expert(q, part, ks):
        at = pl.ds(pl.multiple_of(q * 4 * CAP + part * 2 * CAP, 2 * CAP), 2 * CAP)
        for i, k in enumerate(ks):
            to = pl.ds(pl.multiple_of(q * 4 * CAP + part * 2 * CAP + i * BASE, BASE), BASE)
            from_rows = slice(part * BASE, (part + 1) * BASE)
            xs = recv[k, from_rows, 0:D]
            dys = recv[k, from_rows, D:2 * D]
            if shared and part == 1:
                mine = own[pl.ds(k, 1), 0:1, 0:1].reshape(1, 1).astype(BF16)
                xs = xs * mine
                dys = dys * mine
            xt[to, :] = xs
            dyt[to, :] = dys
        a = nn(xt[at, :], w1[...])
        dh = nt(dyt[at, :], w2[...])
        a2 = a * a
        t = jnp.tanh(a * (GELU_C + (GELU_C * GELU_A) * a2))
        half = 0.5 + 0.5 * t
        h = (a * half).astype(BF16)
        slope = half + (0.5 * a) * (1.0 - t * t) * (GELU_C + (3.0 * GELU_C * GELU_A) * a2)
        da = (dh * slope).astype(BF16)
        hid[at, :] = h
        dpre[at, :] = da
        y = nn(h, w2[...]).astype(BF16)
        dx = nt(da, w1[...]).astype(BF16)
        for i, k in enumerate(ks):
            ys[k, part * BASE:(part + 1) * BASE, :] = y[i * BASE:(i + 1) * BASE]
            dxs[k, part * BASE:(part + 1) * BASE, :] = dx[i * BASE:(i + 1) * BASE]

    for c in loads[4:]:
        c.wait()
    if shared:
        @pl.loop(1, N)
        def _(k):
            flag_copy(k).wait_recv()

    if shared:
        seen = own[0]
        for k in range(1, N):
            seen = seen + own[k]
        full[0, 0] = jnp.max(seen[:, 64:128])
    else:
        full[0, 0] = 0.0

    @pl.loop(0, STEPS)
    def _(q):
        ja, jb = chips_of(q)
        ks = (2 * ja, 2 * ja + 1, 2 * jb, 2 * jb + 1)

        if shared:
            @pl.when(q > 0)
            def _():
                in_over(ja).wait_recv()
                pass_on(ja).start()

            in_over(jb).wait_recv()
            pass_on(jb).start()

        @pl.when(q > 0)
        def _():
            in_copy(ks[0]).wait_recv()

        for k in ks[1:]:
            in_copy(k).wait_recv()
        expert(q, 0, ks)
        if not shared:
            expert(q, 1, ks)

        @pl.when(q > 0)
        def _():
            y_copy(ks[0]).start()

        for k in ks[1:]:
            y_copy(k).start()
        if shared:
            @pl.when(q > 0)
            def _():
                for j in chips_of(q - 1):
                    merge(j)

                @pl.when(q > 1)
                def _():
                    y_over(chips_of(q - 1)[0]).start()

                y_over(chips_of(q - 1)[1]).start()

            for j in (ja, jb):
                pass_on(j).wait_recv()
            expert(q, 1, ks)
            for j in (ja, jb):
                y_merge(j).start()
                dx_merge(j).start()

    if shared:
        for j in chips_of(STEPS - 1):
            merge(j)
            y_over(j).start()

    def send_dx(q):
        for j in chips_of(q):
            def even(j=j):
                dx_copy(2 * j).start()
                if shared:
                    dx_over(j).start()

            if isinstance(j, int):
                even()
            else:
                pl.when(j > 0)(even)

            dx_copy(2 * j + 1).start()

    @pl.loop(0, STEPS // 2)
    def _(q):
        send_dx(q)

    yr[0, 0:rows, :] = ys[0, 0:rows, :]
    dxr[0, 0:rows, :] = dxs[0, 0:rows, :]
    if shared:
        yr[0, BASE:2 * BASE, :] = yo[0]
        dxr[0, BASE:2 * BASE, :] = dxo[0]

    lane_f = lax.broadcasted_iota(jnp.int32, (TOK, CAP), 1).astype(F32)
    lane_i = lax.broadcasted_iota(jnp.int32, (TOK, 128), 1)

    def picks(k):
        return jnp.where(slot_col[k] == lane_f, 1.0, 0.0).astype(BF16)

    @pl.loop(0, CHIPS)
    def _(p):
        ja, jb = chips_of(lax.div(p, 2))
        j = ja + lax.rem(p, 2) * (jb - ja)

        @pl.when(j > 0)
        def _():
            y_copy(2 * j).wait_recv()
            if shared:
                y_over(j).wait_recv()

        y_copy(2 * j + 1).wait_recv()
        if shared:
            yr[2 * j + 1, BASE:2 * BASE, :] = yr[2 * j, BASE:2 * BASE, :]
        for c in range(2):
            k = 2 * j + c
            zy = nn(picks(k), yr[k])
            gc = gate_col[k]
            acc_y[:, 0:128] += gc * zy[:, 0:128]
            acc_y[:, 128:256] += gc * zy[:, 128:256]
            dg = jnp.sum(zy * do_ref[...].astype(F32), axis=1, keepdims=True)
            acc_dg[...] += jnp.where(lane_i == k, dg, 0.0)

    gmat = jnp.concatenate([gates_t, jnp.zeros((TOK, 128 - N), F32)], axis=1)
    dgm = acc_dg[...]
    mean = jnp.sum(gmat * dgm, axis=1, keepdims=True)
    dl = (gmat * (dgm - mean)).astype(BF16)

    part = tn(dl, x_ref[...])
    for k in range(N):
        gpart[k] = part[k:k + 1, :]

    def part_copy(k):
        return remote(here, gpart.at[k], grecv.at[k], g_s.at[k], g_r.at[k], k)

    def sum_copy(k):
        return remote(here, gall.at[me], gall.at[me], a_s.at[k], a_r.at[k], k)

    @pl.loop(1, N)
    def _(k):
        part_copy(k).start()

    send_dx(2)
    send_dx(3)

    @pl.loop(0, H // 256)
    def _(c):
        cols = pl.ds(pl.multiple_of(c * 256, 256), 256)
        gwi[:, cols] = tn(xt[...], dpre[:, cols])

    @pl.loop(0, H // 256)
    def _(c):
        cols = pl.ds(pl.multiple_of(c * 256, 256), 256)
        gwo[cols, :] = jnp.transpose(tn(dyt[...], hid[:, cols]))

    @pl.loop(1, N)
    def _(k):
        part_copy(k).wait_recv()

    total = gpart[0]
    for k in range(1, N):
        total = total + grecv[k]
    gall[me] = total

    @pl.loop(1, N)
    def _(k):
        sum_copy(k).start()

    y_ref[...] = acc_y[...].astype(BF16)
    perm_r = lax.broadcasted_iota(jnp.int32, (128, N), 0)
    perm_c = lax.broadcasted_iota(jnp.int32, (128, N), 1)
    perm = jnp.where(jnp.bitwise_xor(perm_c, me) == perm_r, 1.0, 0.0).astype(BF16)
    d_log = nn(dl, perm).astype(BF16)
    gate_part = nn(d_log, wg_ref[...])

    @pl.loop(1, N)
    def _(k):
        in_copy(k).wait_send()
        y_copy(k).wait_send()
        part_copy(k).wait_send()
        if shared:
            flag_copy(k).wait_send()

    if shared:
        @pl.loop(0, CHIPS)
        def _(j):
            pass_on(j).wait_send()
            y_merge(j).wait_send()
            dx_merge(j).wait_send()

            @pl.when(j > 0)
            def _():
                in_over(j).wait_send()
                y_over(j).wait_send()

    @pl.loop(0, CHIPS)
    def _(p):
        ja, jb = chips_of(lax.div(p, 2))
        j = ja + lax.rem(p, 2) * (jb - ja)

        @pl.when(j > 0)
        def _():
            dx_copy(2 * j).wait_send()
            dx_copy(2 * j).wait_recv()
            if shared:
                dx_over(j).wait_send()
                dx_over(j).wait_recv()

        dx_copy(2 * j + 1).wait_send()
        dx_copy(2 * j + 1).wait_recv()
        if shared:
            dxr[2 * j + 1, BASE:2 * BASE, :] = dxr[2 * j, BASE:2 * BASE, :]
        sel = jnp.concatenate([picks(2 * j), picks(2 * j + 1)], axis=1)
        acc_dx[...] += nn(sel, dxr[pl.ds(2 * j, 2)].reshape(2 * CAP, D))

    gx_ref[...] = (acc_dx[...] + gate_part).astype(BF16)

    @pl.loop(1, N)
    def _(k):
        pr = peer_of(*here, k)
        remote(here, gall.at[pr], gall.at[pr], a_s.at[k], a_r.at[k], k).wait_recv()

    for e in range(N):
        gwg_ref[e:e + 1, :] = gall[e]

    @pl.loop(1, N)
    def _(k):
        sum_copy(k).wait_send()


def write_out(*refs):
    sem = refs[10]
    copies = [pltpu.make_async_copy(refs[i], refs[5 + i], sem.at[i]) for i in range(5)]
    for c in copies:
        c.start()
    for c in copies:
        c.wait()


RESULTS = (((TOK, D), BF16), ((TOK, D), BF16), ((D, H), F32), ((H, D), F32), ((N, D), F32))


def run_block(shared, *args):
    vm = pl.BlockSpec(memory_space=pltpu.VMEM)
    anyspace = pl.BlockSpec(memory_space=pl.ANY)
    dma = pltpu.SemaphoreType.DMA
    rows = BASE if shared else CAP
    over = BASE if shared else 8
    return pl.pallas_call(
        functools.partial(block, shared),
        out_shape=tuple(pltpu.VMEM(shape, dtype) for shape, dtype in RESULTS) + (pltpu.SMEM((1, 1), F32),),
        in_specs=[anyspace] * 6,
        out_specs=(vm,) * 5 + (pl.BlockSpec(memory_space=pltpu.SMEM),),
        scratch_shapes=[
            pltpu.VMEM((TOK, D), BF16),
            pltpu.VMEM((2, TOK), jnp.int32),
            pltpu.VMEM((N, D), BF16),
            pltpu.VMEM((TOK, D), BF16),
            pltpu.VMEM((D, H), BF16),
            pltpu.VMEM((H, D), BF16),
            pltpu.VMEM((N, TOK), F32),
            pltpu.VMEM((N, TOK), F32),
            pltpu.VMEM((N, 1, 128), F32),
            pltpu.VMEM((N, 1, 128), F32),
            pltpu.VMEM((4 * CAP, TOK), BF16),
            pltpu.VMEM((N, rows, 2 * D), BF16),
            pltpu.VMEM((CHIPS, over, 2 * D), BF16),
            pltpu.VMEM((N, CAP, 2 * D), BF16),
            pltpu.VMEM((N * CAP, D), BF16),
            pltpu.VMEM((N * CAP, D), BF16),
            *[pltpu.VMEM((N, CAP, D), BF16)] * 4,
            *[pltpu.VMEM((CHIPS, over, D), BF16)] * 4,
            pltpu.VMEM((N * CAP, H), BF16),
            pltpu.VMEM((N * CAP, H), BF16),
            pltpu.VMEM((N, TOK, 128), F32),
            pltpu.VMEM((N, TOK, 128), F32),
            pltpu.VMEM((TOK, D), F32),
            pltpu.VMEM((TOK, D), F32),
            pltpu.VMEM((TOK, 128), F32),
            *[pltpu.VMEM((N, 1, D), F32)] * 3,
            *[dma((N,))] * 2,
            *[dma((CHIPS,))] * 4,
            *[dma((N,))] * 2,
            *[dma((CHIPS,))] * 2,
            *[dma((N,))] * 2,
            *[dma((CHIPS,))] * 6,
            *[dma((N,))] * 6,
            dma((6,)),
        ],
        compiler_params=pltpu.CompilerParams(collective_id=0 if shared else 1, has_side_effects=True, vmem_limit_bytes=56 * 2 ** 20),
    )(*args)


def finish(*raw):
    vm = pl.BlockSpec(memory_space=pltpu.VMEM)
    anyspace = pl.BlockSpec(memory_space=pl.ANY)
    return pl.pallas_call(
        write_out,
        out_shape=tuple(jax.ShapeDtypeStruct(shape, dtype) for shape, dtype in RESULTS),
        in_specs=[vm] * 5,
        out_specs=(anyspace,) * 5,
        scratch_shapes=[pltpu.SemaphoreType.DMA((5,))],
        compiler_params=pltpu.CompilerParams(vmem_limit_bytes=2 ** 20),
    )(*[pltpu.with_memory_space_constraint(r, pltpu.VMEM) for r in raw])


def local_block(tokens, grad_out, expert_ids, w_gate, w_in, w_out):
    args = (tokens, expert_ids.T, w_gate.T, grad_out, w_in[0], w_out[0])
    args = tuple(pltpu.with_memory_space_constraint(v, pltpu.HBM) for v in args)
    *raw, full = run_block(True, *args)
    raw = [pltpu.with_memory_space_constraint(r, pltpu.VMEM) for r in raw]
    y, gx, gwi, gwo, gwg = lax.cond(
        full[0, 0] > 0.5,
        lambda raw, args: finish(*run_block(False, *args)[:5]),
        lambda raw, args: finish(*raw),
        raw, args)
    return y, gx, gwi[None], gwo[None], gwg.T


def solution(mesh):
    return jax.shard_map(local_block, mesh=mesh, in_specs=(P('ep'), P('ep'), P('ep'), P(), P('ep'), P('ep')), out_specs=(P('ep'), P('ep'), P('ep'), P('ep'), P()), check_vma=False)
```
